128 devices in a mesh: owner: 4 (over x), rows: 32 (over z, y, core).
Axes of the slice: x: 4, y: 4, z: 4, core: 2. Of those that a mesh axis runs over, the one named last changes fastest.
Arguments:
- w_gate: float32 [64, 2048, 1024], P('owner', 'rows'), may hold values from -0.25 to 0.25
- avg_gate: bfloat16 [64, 2048, 1024], P('owner', 'rows'), may hold values from -0.0625 to 0.0625
- w_up: float32 [64, 2048, 1024], P('owner', 'rows'), may hold values from -0.25 to 0.25
- avg_up: bfloat16 [64, 2048, 1024], P('owner', 'rows'), may hold values from -0.0625 to 0.0625
- w_down: float32 [64, 1024, 2048], P('owner', None, 'rows'), may hold values from -0.375 to 0.375
- avg_down: bfloat16 [64, 1024, 2048], P('owner', None, 'rows'), may hold values from -0.09375 to 0.09375
- router_weight: float32 [2048, 64], P('rows', 'owner'), may hold values from -0.125 to 0.125
- router_gain: float32 [2048], P('rows'), may hold values from 0.25 to 1.75
Outputs:
- serve_gate: bfloat16 [64, 2048, 1024], P('owner', None, 'rows')
- serve_up: bfloat16 [64, 2048, 1024], P('owner', None, 'rows')
- serve_down: bfloat16 [64, 1024, 2048], P('owner', 'rows')
- scale_gate: float32 [64, 1024], P('owner', 'rows')
- scale_up: float32 [64, 1024], P('owner', 'rows')
- scale_down: float32 [64, 1024], P('owner', 'rows')
- serve_router: bfloat16 [2048, 64], replicated
The draws below stay inside these ranges and needn't reach their ends.
All inputs are finite; a program needn't handle non-finite values.
Results may differ from the reference program's by a relative error of at most 0.0015.
Values may be sent and summed in bfloat16 or wider, within the bound.
A program may use at most 128 MiB of HBM per device.

```python
import jax
import jax.numpy as jnp
from jax import lax

EXPERTS = 64
D_MODEL = 2048
D_EXPERT = 1024


def raised(drawn, stream_key, source, target, shards_of, factor):
    owner, partner = [(jnp.arange(drawn.shape[position]) // (drawn.shape[position] // shards_of)).reshape([-1 if axis == position else 1 for axis in range(drawn.ndim)]) for position in (source, target)]
    chosen = jax.random.permutation(stream_key, shards_of)[partner]
    strong = (owner == chosen) | (owner == (partner + shards_of // 2) % shards_of)
    return jnp.where(strong, factor * drawn, drawn)


def shard_levels(key, dims, shards, smallest, top_value):
    factor_of = 1.0
    for position, blocks in shards:
        draws = jax.random.uniform(jax.random.fold_in(jax.random.fold_in(key, 6), position), (blocks,), jnp.float32, smallest / len(shards), top_value / len(shards))
        factor_of = factor_of * jnp.repeat(jnp.exp(draws), dims[position] // blocks).reshape((-1,) + (1,) * (len(dims) - 1 - position))
    return factor_of


def centred(own_key, dims, spread, limit, pieces=(), held_as=jnp.bfloat16):
    factor_of = shard_levels(own_key, dims, pieces, -0.22, 0.18) if pieces else 1.0
    entries = jax.random.normal(own_key, dims, jnp.float32) * spread * factor_of
    return jnp.minimum(jnp.maximum(entries, -limit), limit).astype(held_as)


def noise_with(stream_key, shape, deviation, limit, cuts, heavy, dtype=jnp.bfloat16):
    result = deviation * jax.random.normal(stream_key, shape, jnp.float32)
    if cuts:
        result = result * shard_levels(stream_key, shape, cuts, -0.22, 0.18)
    return jnp.clip(raised(result, jax.random.fold_in(stream_key, 3), *heavy), -limit, limit).astype(dtype)


def setup_inputs(seed: int = 0) -> dict:
    streams_of = jax.random.split(jax.random.key(seed), 9)
    w_gate = noise_with(streams_of[0], (EXPERTS, D_MODEL, D_EXPERT), D_MODEL ** -0.5, 0.25, ((0, 4), (1, 32)), (1, 2, 32, 2.75), jnp.float32)
    avg_gate = centred(streams_of[1], (EXPERTS, D_MODEL, D_EXPERT), (D_MODEL * 4) ** -0.5, 0.0625, ((0, 4), (1, 32)))
    w_up = noise_with(streams_of[2], (EXPERTS, D_MODEL, D_EXPERT), D_MODEL ** -0.5, 0.25, ((0, 4), (1, 32)), (1, 2, 32, 2.75), jnp.float32)
    avg_up = centred(streams_of[3], (EXPERTS, D_MODEL, D_EXPERT), (D_MODEL * 4) ** -0.5, 0.0625, ((0, 4), (1, 32)))
    w_down = noise_with(streams_of[4], (EXPERTS, D_EXPERT, D_MODEL), D_EXPERT ** -0.5, 0.375, ((0, 4), (2, 32)), (2, 1, 32, 2.75), jnp.float32)
    avg_down = centred(streams_of[5], (EXPERTS, D_EXPERT, D_MODEL), (D_EXPERT * 4) ** -0.5, 0.09375, ((0, 4), (2, 32)))
    router_weight = centred(streams_of[6], (D_MODEL, EXPERTS), D_MODEL ** -0.5, 0.125, ((0, 32), (1, 4)), jnp.float32)
    router_gain = jnp.clip(1.0 + 0.15 * jax.random.normal(streams_of[7], (D_MODEL,), jnp.float32), 0.25, 1.75)
    return {"w_gate": w_gate, "avg_gate": avg_gate, "w_up": w_up, "avg_up": avg_up, "w_down": w_down, "avg_down": avg_down, "router_weight": router_weight, "router_gain": router_gain}


def reference(w_gate, avg_gate, w_up, avg_up, w_down, avg_down, router_weight, router_gain):
    fresh_gate = w_gate + avg_gate.astype(jnp.float32)
    fresh_up = w_up + avg_up.astype(jnp.float32)
    fresh_down = w_down + avg_down.astype(jnp.float32)
    scale_gate = jnp.sqrt(lax.optimization_barrier(jnp.sum(fresh_gate * fresh_gate, axis=1)))
    serve_gate = (fresh_gate / jnp.expand_dims(scale_gate, 1)).astype(jnp.bfloat16)
    scale_up = jnp.sqrt(lax.optimization_barrier(jnp.sum(fresh_up * fresh_up, axis=1)))
    serve_up = (fresh_up / jnp.expand_dims(scale_up, 1)).astype(jnp.bfloat16)
    scale_down = jnp.sqrt(lax.optimization_barrier(jnp.sum(fresh_down * fresh_down, axis=2)))
    serve_down = (fresh_down / jnp.expand_dims(scale_down, 2)).astype(jnp.bfloat16)
    serve_router = (router_weight * router_gain[:, None]).astype(jnp.bfloat16)
    return (serve_gate, serve_up, serve_down, scale_gate, scale_up, scale_down, serve_router)
```

```python
import functools

import jax
import jax.numpy as jnp
from jax import lax
from jax.experimental import pallas as pl
from jax.experimental.pallas import tpu as pltpu
from jax.sharding import PartitionSpec as P

MESH = pl.DeviceIdType.MESH
F32, BF16 = jnp.float32, jnp.bfloat16

SIDE = 4
CHIPS = 16
HALF = 8
JOBS = 24
BLOCKS = 8
PAIR = 2

GROUPS = ((0, 2, True), (2, 2, True), (4, 4, False), (8, 8, False), (16, 8, False))


def exchange(*refs):
    (w_gate, a_gate, w_up, a_up, w_down, a_down, r_weight, r_gain) = refs[:8]
    (o_gate, o_up, o_down, o_scale, o_router) = refs[8:13]
    (wide, narrow, ready, scale, inverse, all0, all1, part2, got2, sum2, part3, got3, sum3, part4, got4, sum4) = refs[13:29]
    (rw, rg, tile, load_sem, trade_out, trade_in, sum_out, sum_in, tot_in, ready_sem, done_sem, route_out, route_in, line_in, scale_sem) = refs[29:]
    weights, changes, outs = (w_gate, w_up, w_down), (a_gate, a_up, a_down), (o_gate, o_up, o_down)
    owner, row = lax.axis_index("owner"), lax.axis_index("rows")
    chip, core = row // 2, row % 2
    z, y = chip // SIDE, chip % SIDE
    other = 1 - core
    partner = (owner, chip * 2 + other)

    def chip_at(k):
        return (z + k // SIDE) % SIDE * SIDE + (y + k % SIDE) % SIDE

    def rows_of(which):
        return pl.ds(pl.multiple_of(which * 64, 64), 64)

    def loads(g):
        first, n, _ = GROUPS[g]
        m, e = first // HALF, first % HALF
        jobs = pl.ds(first, n)
        return [
            pltpu.make_async_copy(
                src.at[pl.ds(core * HALF + e, n)], dst.at[jobs, rows_of(core), :], load_sem.at[g, i]
            )
            for i, (src, dst) in enumerate(((weights[m], wide), (changes[m], narrow)))
        ]

    def trades(g):
        first, n, _ = GROUPS[g]
        m, e = first // HALF, first % HALF
        jobs = pl.ds(first, n)
        return [
            pltpu.make_async_remote_copy(
                src_ref=src.at[pl.ds(other * HALF + e, n)],
                dst_ref=dst.at[jobs, rows_of(core), :],
                send_sem=trade_out.at[g, i],
                recv_sem=trade_in.at[g, i],
                device_id=partner,
                device_id_type=MESH,
            )
            for i, (src, dst) in enumerate(((weights[m], wide), (changes[m], narrow)))
        ]

    route_local = [
        pltpu.make_async_copy(r_weight, rw.at[core], load_sem.at[len(GROUPS), 0]),
        pltpu.make_async_copy(r_gain, rg.at[core], load_sem.at[len(GROUPS), 1]),
    ]
    route_trade = [
        pltpu.make_async_remote_copy(
            src_ref=src, dst_ref=dst.at[core], send_sem=trade_out.at[len(GROUPS), i],
            recv_sem=trade_in.at[len(GROUPS), i], device_id=partner, device_id_type=MESH,
        )
        for i, (src, dst) in enumerate(((r_weight, rw), (r_gain, rg)))
    ]

    for g in range(len(GROUPS)):
        for copy in loads(g):
            copy.start()
    for copy in route_local:
        copy.start()

    barrier = pltpu.get_barrier_semaphore()
    pl.semaphore_signal(barrier, inc=1, device_id=partner, device_id_type=MESH)

    def greet(k, carry):
        for c in range(2):
            pl.semaphore_signal(
                barrier, inc=1, device_id=(owner, chip_at(k) * 2 + c), device_id_type=MESH
            )
        return carry

    lax.fori_loop(1, CHIPS, greet, 0)
    for k in range(1, SIDE):
        for c in range(2):
            pl.semaphore_signal(
                barrier, inc=1, device_id=((owner + k) % SIDE, chip * 2 + c), device_id_type=MESH
            )
    pl.semaphore_wait(barrier, 1 + 2 * (CHIPS - 1) + 2 * (SIDE - 1))

    for copy in trades(0) + trades(1) + route_trade:
        copy.start()
    for g in range(2, len(GROUPS)):
        for copy in trades(g):
            copy.start()

    def arrived(g):
        for copy in loads(g):
            copy.wait()
        for copy in trades(g):
            copy.wait_recv()

    def fresh(job, b):
        lanes = slice(b * 128, (b + 1) * 128)
        return wide[job, :, lanes] + narrow[job, :, lanes].astype(F32)

    def square_sum(job, b):
        x = fresh(job, b)
        return jnp.sum(x * x, axis=0, keepdims=True)

    def to_chips(src, dst, out_sem, in_sem):
        def go(k, carry):
            there = chip_at(k)
            pltpu.make_async_remote_copy(
                src_ref=src(there), dst_ref=dst, send_sem=out_sem, recv_sem=in_sem,
                device_id=(owner, there * 2 + core), device_id_type=MESH,
            ).start()
            return carry

        lax.fori_loop(1, CHIPS, go, 0)

    def wait_for(ref, sem):
        pltpu.make_async_copy(ref, ref, sem).wait()

    def keep(job, b, total):
        root = jnp.sqrt(total)
        scale[job, b] = root
        inverse[job, b] = 1.0 / root

    def sums_broadcast(g, got):
        first, n, _ = GROUPS[g]
        for i in range(n):
            for b in range(BLOCKS):
                got[chip, i, b : b + 1, :] = square_sum(first + i, b)
        to_chips(lambda there: got.at[chip], got.at[chip], sum_out.at[g], sum_in.at[g])

    def sums_added(g, got):
        first, n, _ = GROUPS[g]
        wait_for(got.at[pl.ds(0, CHIPS - 1)], sum_in.at[g])
        for i in range(n):
            total = got[0, i]
            for s in range(1, CHIPS):
                total = total + got[s, i]
            for b in range(BLOCKS):
                keep(first + i, b, total[b : b + 1, :])

    def sums_scattered(g, part, got):
        first, n, _ = GROUPS[g]
        per = n // 2

        def one(i, carry):
            for b in range(BLOCKS):
                line = i * BLOCKS + b
                part[line // per, line % per] = square_sum(first + i, b)
            return carry

        lax.fori_loop(0, n, one, 0)
        got[chip] = part[chip]
        to_chips(lambda there: part.at[there], got.at[chip], sum_out.at[g], sum_in.at[g])

    def sums_gathered(g, got, whole):
        wait_for(got.at[pl.ds(0, CHIPS - 1)], sum_in.at[g])
        total = got[0]
        for s in range(1, CHIPS):
            total = total + got[s]
        whole[chip] = total
        to_chips(lambda there: whole.at[chip], whole.at[chip], ready_sem.at[g], tot_in.at[g])

    def sums_taken(g, whole):
        first, n, _ = GROUPS[g]
        per = n // 2
        wait_for(whole.at[pl.ds(0, CHIPS - 1)], tot_in.at[g])

        def one(i, carry):
            for b in range(BLOCKS):
                line = i * BLOCKS + b
                keep(first + i, b, whole[line // per, line % per])
            return carry

        lax.fori_loop(0, n, one, 0)

    mine = pl.ds(pl.multiple_of(chip * 128, 128), 128)

    def send(out, at, job):
        for i in range(PAIR):

            def blocks(b, carry, i=i):
                lanes = pl.ds(pl.multiple_of(b * 128, 128), 128)
                x = wide[job + i, :, lanes] + narrow[job + i, :, lanes].astype(F32)
                x = x * inverse[job + i, b]
                ready[job + i, lanes, :] = x.T.astype(BF16)
                return carry

            lax.fori_loop(0, BLOCKS, blocks, 0)

        def go(k, carry):
            there = chip_at(CHIPS - k)
            for t in range(2):
                row_there = there * 2 + (core + t) % 2
                pltpu.make_async_remote_copy(
                    src_ref=ready.at[pl.ds(job, PAIR), pl.ds(pl.multiple_of(row_there * 32, 32), 32), :],
                    dst_ref=out.at[pl.ds(at, PAIR), :, mine],
                    send_sem=done_sem.at[0],
                    recv_sem=done_sem.at[1],
                    device_id=(owner, row_there),
                    device_id_type=MESH,
                ).start()
            return carry

        lax.fori_loop(1, CHIPS, go, 0)
        row_there = chip * 2 + other
        pltpu.make_async_remote_copy(
            src_ref=ready.at[pl.ds(job, PAIR), pl.ds(pl.multiple_of(row_there * 32, 32), 32), :],
            dst_ref=out.at[pl.ds(at, PAIR), :, mine],
            send_sem=done_sem.at[0],
            recv_sem=done_sem.at[1],
            device_id=partner,
            device_id_type=MESH,
        ).start()
        for i in range(PAIR):
            out[at + i, :, mine] = ready[job + i, pl.ds(pl.multiple_of(row * 32, 32), 32), :]

    def sends(first, n):
        m, e = first // HALF, first % HALF

        def one(i, carry):
            send(outs[m], core * HALF + e + i * PAIR, first + i * PAIR)
            return carry

        lax.fori_loop(0, n // PAIR, one, 0)

    def router_tile():
        for copy in route_local:
            copy.wait()
        for copy in route_trade:
            copy.wait_recv()
        folded = jnp.concatenate([rw[c] * rg[c] for c in range(2)], axis=1).astype(BF16)
        tile[...] = folded
        for_core = pl.ds(pl.multiple_of(core * HALF, HALF), HALF)
        lines = pl.ds(pl.multiple_of(owner * 16 + core * HALF, HALF), HALF)
        o_router[lines, mine] = jnp.where(core == 0, folded[:HALF], folded[HALF:])
        to_chips(lambda there: tile.at[for_core], o_router.at[lines, mine], route_out.at[0], route_in.at[0])

    lines = pl.ds(pl.multiple_of(owner * 16 + core * HALF, HALF), HALF)

    def router_lines():
        wait_for(o_router.at[pl.ds(0, HALF), pl.ds(0, 15 * 128)], route_in.at[0])
        for k in range(SIDE):
            for c in range(2):
                if k == 0 and c == 0:
                    continue
                to = ((owner + k) % SIDE, chip * 2 + (core + c) % 2)
                pltpu.make_async_remote_copy(
                    src_ref=o_router.at[lines, :], dst_ref=o_router.at[lines, :], send_sem=route_out.at[1],
                    recv_sem=line_in.at[0], device_id=to, device_id_type=MESH,
                ).start()

    arrived(0)
    sums_broadcast(0, all0)
    arrived(1)
    sums_broadcast(1, all1)
    router_tile()
    arrived(2)
    sums_scattered(2, part2, got2)
    sums_added(0, all0)
    sends(0, 2)
    sums_gathered(2, got2, sum2)
    sums_added(1, all1)
    sends(2, 2)
    arrived(3)
    sums_scattered(3, part3, got3)
    sums_taken(2, sum2)
    sends(4, 2)
    sums_gathered(3, got3, sum3)
    router_lines()
    sends(6, 2)
    arrived(4)
    sums_scattered(4, part4, got4)
    sums_taken(3, sum3)
    sends(8, 2)
    sums_gathered(4, got4, sum4)
    sends(10, 6)
    sums_taken(4, sum4)
    sends(16, 8)

    for b in range(1):
        o_scale[core] = scale[:, chip // 2]
        share = pltpu.make_async_remote_copy(
            src_ref=scale.at[:, chip // 2], dst_ref=o_scale.at[core], send_sem=scale_sem.at[0],
            recv_sem=scale_sem.at[1], device_id=partner, device_id_type=MESH,
        )
        share.start()

    for g, (first, n, _) in enumerate(GROUPS):
        for copy in trades(g):
            copy.wait_send()
    for copy in route_trade:
        copy.wait_send()
    for g, got in enumerate((all0, all1, got2, got3, got4)):
        wait_for(got.at[pl.ds(0, CHIPS - 1)], sum_out.at[g])
    for g, whole in ((2, sum2), (3, sum3), (4, sum4)):
        wait_for(whole.at[pl.ds(0, CHIPS - 1)], ready_sem.at[g])
    wait_for(o_router.at[pl.ds(0, HALF), pl.ds(0, 15 * 128)], route_out.at[0])
    for _ in range(7):
        wait_for(o_router.at[pl.ds(0, HALF), :], route_out.at[1])
    wait_for(o_router.at[pl.ds(0, 56), :], line_in.at[0])
    share.wait()
    for s in range(2):
        wait_for(ready.at[:, pl.ds(0, 31 * 32), :], done_sem.at[s])


def write_out(*refs):
    (gate, up, down, scale, router, o_gate, o_up, o_down, s_gate, s_up, s_down, o_router, sem) = refs
    copies = [
        pltpu.make_async_copy(src, dst, sem.at[i])
        for i, (src, dst) in enumerate(((gate, o_gate), (up, o_up), (down, o_down), (router, o_router)))
    ]
    for copy in copies:
        copy.start()
    row = lax.axis_index("rows")
    for m, out in enumerate((s_gate, s_up, s_down)):
        for c in range(2):
            block = scale[c, m * HALF : (m + 1) * HALF, 0, :]
            block = pltpu.roll(block, (128 - row % 4 * 32) % 128, 1)
            out[c * HALF : (c + 1) * HALF, :] = block[:, :32]
    for copy in copies:
        copy.wait()


def shards(w_gate, avg_gate, w_up, avg_up, w_down, avg_down, router_weight, router_gain):
    vmem, dma = pltpu.VMEM, pltpu.SemaphoreType.DMA
    hbm = pl.BlockSpec(memory_space=pltpu.HBM)
    anywhere = pl.BlockSpec(memory_space=pltpu.VMEM)
    served = (16, 32, 2048)
    gate, up, down, scale, router = pl.pallas_call(
        exchange,
        out_shape=[
            pltpu.VMEM(served, BF16), pltpu.VMEM(served, BF16), pltpu.VMEM(served, BF16),
            pltpu.VMEM((2, JOBS, 1, 128), F32), pltpu.VMEM((64, 2048), BF16),
        ],
        in_specs=[hbm] * 8,
        out_specs=[anywhere] * 5,
        scratch_shapes=[
            vmem((JOBS, 128, 1024), F32), vmem((JOBS, 128, 1024), BF16), vmem((JOBS, 1024, 128), BF16),
            vmem((JOBS, BLOCKS, 1, 128), F32), vmem((JOBS, BLOCKS, 1, 128), F32),
            vmem((CHIPS, 2, BLOCKS, 128), F32), vmem((CHIPS, 2, BLOCKS, 128), F32),
        ]
        + [vmem((CHIPS, n, 1, 128), F32) for n in (2, 2, 2, 4, 4, 4, 4, 4, 4)]
        + [
            vmem((2, 16, 64), F32), vmem((2, 1, 64), F32), vmem((16, 128), BF16),
            dma((6, 2)), dma((6, 2)), dma((6, 2)), dma((5,)), dma((5,)), dma((5,)), dma((5,)), dma((2,)),
            dma((2,)), dma((2,)), dma((1,)), dma((2,)),
        ],
        compiler_params=pltpu.CompilerParams(
            collective_id=0, has_side_effects=True, vmem_limit_bytes=48 << 20
        ),
        name="exchange",
    )(
        w_gate, avg_gate, w_up, avg_up, jnp.swapaxes(w_down, 1, 2), jnp.swapaxes(avg_down, 1, 2),
        router_weight.T, router_gain[None, :],
    )
    out = pl.BlockSpec(memory_space=pl.ANY)
    small = pl.BlockSpec(memory_space=pltpu.VMEM)
    gate, up, down, s_gate, s_up, s_down, router = pl.pallas_call(
        write_out,
        out_shape=[jax.ShapeDtypeStruct(served, BF16)] * 3
        + [jax.ShapeDtypeStruct((16, 32), F32)] * 3
        + [jax.ShapeDtypeStruct((64, 2048), BF16)],
        in_specs=[small] * 5,
        out_specs=[out] * 3 + [small] * 3 + [out],
        scratch_shapes=[dma((4,))],
        compiler_params=pltpu.CompilerParams(vmem_limit_bytes=8 << 20),
        name="write_out",
    )(*(pltpu.with_memory_space_constraint(x, pltpu.VMEM) for x in (gate, up, down, scale, router)))
    return (
        jnp.swapaxes(gate, 1, 2), jnp.swapaxes(up, 1, 2), down, s_gate, s_up, s_down, router.T,
    )


def solution(mesh):
    return jax.shard_map(
        shards,
        mesh=mesh,
        in_specs=(
            P("owner", "rows", None),
            P("owner", "rows", None),
            P("owner", "rows", None),
            P("owner", "rows", None),
            P("owner", None, "rows"),
            P("owner", None, "rows"),
            P("rows", "owner"),
            P("rows"),
        ),
        out_specs=(
            P("owner", None, "rows"),
            P("owner", None, "rows"),
            P("owner", "rows", None),
            P("owner", "rows"),
            P("owner", "rows"),
            P("owner", "rows"),
            P(),
        ),
        check_vma=False,
    )
```

```python
import jax
import jax.numpy as jnp
from jax import lax
from jax.experimental import pallas as pl
from jax.experimental.pallas import tpu as pltpu
from jax.sharding import PartitionSpec as P

MESH = pl.DeviceIdType.MESH
F32, BF16 = jnp.float32, jnp.bfloat16

SIDE = 4
CHIPS = 16
HALF = 8
JOBS = 24
BLOCKS = 8

LOADS = ((0, 2), (2, 2), (4, 4), (8, 8), (16, 8))
SUMS = ((0, 2), (2, 2), (4, 4), (8, 16))


def exchange(*refs):
    (w_gate, a_gate, w_up, a_up, w_down, a_down, r_weight, r_gain) = refs[:8]
    (o_gate, o_up, o_down, o_scale, o_router) = refs[8:13]
    (wide, narrow, ready, scale, inverse, near_w, near_a, kept, given, taken) = refs[13:23]
    (all0, all1, part2, got2, sum2, part3, got3, sum3) = refs[23:31]
    (rw, rg, tile, load_sem, near_sem, trade_out, trade_in, sum_out, sum_in, ready_sem, tot_in,
     done_sem, route_sem, line_sem, scale_sem, near_share) = refs[31:]
    weights, changes, outs = (w_gate, w_up, w_down), (a_gate, a_up, a_down), (o_gate, o_up, o_down)
    owner, row = lax.axis_index("owner"), lax.axis_index("rows")
    chip, core = row // 2, row % 2
    z, y = chip // SIDE, chip % SIDE
    other = 1 - core
    partner_row = chip * 2 + other
    partner = (owner, partner_row)

    def chip_at(k):
        return (z + k // SIDE) % SIDE * SIDE + (y + k % SIDE) % SIDE

    def rows_of(which):
        return pl.ds(pl.multiple_of(which * 64, 64), 64)

    def to_partner(src, dst, out_sem, in_sem):
        return pltpu.make_async_remote_copy(
            src_ref=src, dst_ref=dst, send_sem=out_sem, recv_sem=in_sem, device_id=partner,
            device_id_type=MESH,
        )

    def sources(g):
        first, n = LOADS[g]
        m, e = first // HALF, first % HALF
        return first, n, e, ((weights[m], wide), (changes[m], narrow))

    def loads(g):
        first, n, e, pairs = sources(g)
        return [
            pltpu.make_async_copy(
                src.at[pl.ds(core * HALF + e, n)], dst.at[pl.ds(first, n), rows_of(core), :], load_sem.at[g, i]
            )
            for i, (src, dst) in enumerate(pairs)
        ]

    def near_loads(g):
        first, n, e, pairs = sources(g)
        return [
            pltpu.make_async_copy(
                src.at[pl.ds(other * HALF + e, n)], dst.at[pl.ds(first, n)], near_sem.at[g, i]
            )
            for i, ((src, _), dst) in enumerate(zip(pairs, (near_w, near_a)))
        ]

    def trades(g):
        first, n, e, pairs = sources(g)
        return [
            to_partner(
                src.at[pl.ds(other * HALF + e, n)], dst.at[pl.ds(first, n), rows_of(core), :],
                trade_out.at[g, i], trade_in.at[g, i],
            )
            for i, (src, dst) in enumerate(pairs)
        ]

    last = len(LOADS)
    route_local = [
        pltpu.make_async_copy(src, dst.at[core], load_sem.at[last, i])
        for i, (src, dst) in enumerate(((r_weight, rw), (r_gain, rg)))
    ]
    route_trade = [
        to_partner(src, dst.at[core], trade_out.at[last, i], trade_in.at[last, i])
        for i, (src, dst) in enumerate(((r_weight, rw), (r_gain, rg)))
    ]

    for g in range(3):
        for copy in loads(g) + near_loads(g):
            copy.start()
    for copy in route_local:
        copy.start()
    for g in (3, 4):
        for copy in loads(g) + near_loads(g):
            copy.start()

    barrier = pltpu.get_barrier_semaphore()

    def greet(k, carry):
        for c in range(2):
            pl.semaphore_signal(
                barrier, inc=1, device_id=(owner, chip_at(CHIPS - k) * 2 + c), device_id_type=MESH
            )
        return carry

    lax.fori_loop(1, CHIPS, greet, 0)
    for k in range(1, SIDE):
        for c in range(2):
            pl.semaphore_signal(
                barrier, inc=1, device_id=((owner + k) % SIDE, chip * 2 + c), device_id_type=MESH
            )
    pl.semaphore_signal(barrier, inc=1, device_id=partner, device_id_type=MESH)

    def lanes_of(b):
        return slice(b * 128, (b + 1) * 128)

    def squares(x):
        return jnp.sum(x * x, axis=0, keepdims=True)

    def own_rows(g):
        first, n = LOADS[g]
        for copy in loads(g) + near_loads(g):
            copy.wait()

        def one(job, carry):
            for b in range(BLOCKS):
                lanes = lanes_of(b)
                given[job, b : b + 1, :] = squares(near_w[job, :, lanes] + near_a[job, :, lanes].astype(F32))
                kept[job, b : b + 1, :] = squares(
                    wide[job, rows_of(core), lanes] + narrow[job, rows_of(core), lanes].astype(F32)
                )
            return carry

        lax.fori_loop(first, first + n, one, 0)

    def shared(k, first, n):
        jobs = pl.ds(first, n)
        return to_partner(given.at[jobs], taken.at[jobs], near_share.at[k, 0], near_share.at[k, 1])

    near = [shared(0, 0, 8), shared(1, 8, 16)]
    for g in range(3):
        own_rows(g)

    pl.semaphore_wait(barrier, 1 + 2 * (CHIPS - 1) + 2 * (SIDE - 1))

    near[0].start()
    for copy in route_trade + trades(0) + trades(1):
        copy.start()

    def traded(g):
        for copy in trades(g):
            copy.wait_recv()

    def to_chips(src, dst, out_sem, in_sem):
        def go(k, carry):
            there = chip_at(k)
            pltpu.make_async_remote_copy(
                src_ref=src(there), dst_ref=dst, send_sem=out_sem, recv_sem=in_sem,
                device_id=(owner, there * 2 + core), device_id_type=MESH,
            ).start()
            return carry

        lax.fori_loop(1, CHIPS, go, 0)

    def wait_for(ref, sem):
        pltpu.make_async_copy(ref, ref, sem).wait()

    def keep(job, b, total):
        root = jnp.sqrt(total)
        scale[job, b] = root
        inverse[job, b] = 1.0 / root

    def sums_broadcast(g, got):
        first, n = SUMS[g]
        for i in range(n):
            got[chip, i] = kept[first + i] + taken[first + i]
        to_chips(lambda there: got.at[chip], got.at[chip], sum_out.at[g], sum_in.at[g])

    def sums_added(g, got):
        first, n = SUMS[g]
        wait_for(got.at[pl.ds(0, CHIPS - 1)], sum_in.at[g])
        for i in range(n):
            total = got[0, i]
            for s in range(1, CHIPS):
                total = total + got[s, i]
            for b in range(BLOCKS):
                keep(first + i, b, total[b : b + 1, :])

    def sums_scattered(g, part, got):
        first, n = SUMS[g]
        per = n // 2

        def one(i, carry):
            total = kept[first + i] + taken[first + i]
            if n == CHIPS:
                part[i] = total
                return carry
            for b in range(BLOCKS):
                line = i * BLOCKS + b
                part[line // per, line % per] = total[b : b + 1, :]
            return carry

        lax.fori_loop(0, n, one, 0)
        got[chip] = part[chip]
        to_chips(lambda there: part.at[there], got.at[chip], sum_out.at[g], sum_in.at[g])

    def sums_gathered(g, got, whole):
        wait_for(got.at[pl.ds(0, CHIPS - 1)], sum_in.at[g])
        total = got[0]
        for s in range(1, CHIPS):
            total = total + got[s]
        whole[chip] = total
        to_chips(lambda there: whole.at[chip], whole.at[chip], ready_sem.at[g], tot_in.at[g])

    def sums_taken(g, whole):
        first, n = SUMS[g]
        per = n // 2
        wait_for(whole.at[pl.ds(0, CHIPS - 1)], tot_in.at[g])

        def one(i, carry):
            for b in range(BLOCKS):
                line = i * BLOCKS + b
                keep(first + i, b, whole[i, b : b + 1, :] if n == CHIPS else whole[line // per, line % per])
            return carry

        lax.fori_loop(0, n, one, 0)

    mine = pl.ds(pl.multiple_of(chip * 128, 128), 128)

    def lines_for(which):
        return pl.ds(pl.multiple_of(which * 32, 32), 32)

    def to_all(send):
        def go(k, carry):
            there = chip_at(CHIPS - k)
            for t in range(2):
                send(there * 2 + (core + t) % 2)
            return carry

        lax.fori_loop(1, CHIPS, go, 0)
        send(partner_row)

    def normalise(job):
        def blocks(b, carry):
            lanes = pl.ds(pl.multiple_of(b * 128, 128), 128)
            x = wide[job, :, lanes] + narrow[job, :, lanes].astype(F32)
            ready[job, lanes, :] = (x * inverse[job, b]).astype(BF16).T
            return carry

        lax.fori_loop(0, BLOCKS, blocks, 0)

    def issue(m, job):
        at = core * HALF + job - m * HALF

        def send(to):
            pltpu.make_async_remote_copy(
                src_ref=ready.at[job, lines_for(to), :], dst_ref=outs[m].at[at, :, mine],
                send_sem=done_sem.at[0], recv_sem=done_sem.at[1], device_id=(owner, to), device_id_type=MESH,
            ).start()

        to_all(send)
        outs[m][at, :, mine] = ready[job, lines_for(row), :]

    def sends(m, first, n):
        def one(i, carry):
            normalise(first + i)
            issue(m, first + i)
            return carry

        lax.fori_loop(0, n, one, 0)

    lines = pl.ds(pl.multiple_of(owner * 16 + core * HALF, HALF), HALF)

    def router_tile():
        for copy in route_local:
            copy.wait()
        for copy in route_trade:
            copy.wait_recv()
        folded = jnp.concatenate([rw[c] * rg[c] for c in range(2)], axis=1).astype(BF16)
        tile[...] = folded
        for_core = pl.ds(pl.multiple_of(core * HALF, HALF), HALF)
        o_router[lines, mine] = jnp.where(core == 0, folded[:HALF], folded[HALF:])
        to_chips(lambda there: tile.at[for_core], o_router.at[lines, mine], route_sem.at[0], route_sem.at[1])

    def router_lines():
        wait_for(o_router.at[pl.ds(0, HALF), pl.ds(0, 15 * 128)], route_sem.at[1])
        for k in range(SIDE):
            for c in range(2):
                if k == 0 and c == 0:
                    continue
                to = ((owner + k) % SIDE, chip * 2 + (core + c) % 2)
                pltpu.make_async_remote_copy(
                    src_ref=o_router.at[lines, :], dst_ref=o_router.at[lines, :], send_sem=line_sem.at[0],
                    recv_sem=line_sem.at[1], device_id=to, device_id_type=MESH,
                ).start()

    near[0].wait_recv()
    sums_broadcast(0, all0)
    sums_scattered(2, part2, got2)
    sums_broadcast(1, all1)
    own_rows(3)
    own_rows(4)
    near[1].start()
    for copy in trades(2) + trades(3) + trades(4):
        copy.start()
    near[1].wait_recv()
    sums_scattered(3, part3, got3)
    traded(0)
    sums_added(0, all0)
    sends(0, 0, 1)
    sums_gathered(2, got2, sum2)
    sends(0, 1, 1)
    router_tile()
    sums_added(1, all1)
    traded(1)
    sends(0, 2, 1)
    normalise(3)
    sums_gathered(3, got3, sum3)
    issue(0, 3)
    router_lines()
    traded(2)
    sums_taken(2, sum2)
    sends(0, 4, 4)
    traded(3)
    sums_taken(3, sum3)
    sends(1, 8, 8)
    traded(4)
    sends(2, 16, 8)

    o_scale[core] = scale[:, chip // 2]
    share = to_partner(scale.at[:, chip // 2], o_scale.at[core], scale_sem.at[0], scale_sem.at[1])
    share.start()

    for copy in near:
        copy.wait_send()
    for g in range(len(LOADS)):
        for copy in trades(g):
            copy.wait_send()
    for copy in route_trade:
        copy.wait_send()
    for g, got in enumerate((all0, all1, got2, got3)):
        wait_for(got.at[pl.ds(0, CHIPS - 1)], sum_out.at[g])
    for g, whole in ((2, sum2), (3, sum3)):
        wait_for(whole.at[pl.ds(0, CHIPS - 1)], ready_sem.at[g])
    wait_for(o_router.at[pl.ds(0, HALF), pl.ds(0, 15 * 128)], route_sem.at[0])
    for s in range(2):
        wait_for(o_router.at[pl.ds(0, 56), :], line_sem.at[s])
    share.wait()
    for s in range(2):
        wait_for(ready.at[:, pl.ds(0, 31 * 32), :], done_sem.at[s])


def write_out(*refs):
    (gate, up, down, scale, router, o_gate, o_up, o_down, *rest) = refs
    (*o_scales, o_router, lines, sem) = rest
    large = [
        pltpu.make_async_copy(src, dst, sem.at[i])
        for i, (src, dst) in enumerate(((gate, o_gate), (up, o_up), (down, o_down), (router, o_router)))
    ]
    for copy in large:
        copy.start()
    row = lax.axis_index("rows")
    for m in range(3):
        for c in range(2):
            block = scale[c, m * HALF : (m + 1) * HALF, 0, :]
            block = pltpu.roll(block, (128 - row % 4 * 32) % 128, 1)
            lines[m, c * HALF : (c + 1) * HALF, :] = block[:, :32]
    small = [pltpu.make_async_copy(lines.at[m], out, sem.at[4 + m]) for m, out in enumerate(o_scales)]
    for copy in small:
        copy.start()
    for copy in large + small:
        copy.wait()


def shards(w_gate, avg_gate, w_up, avg_up, w_down, avg_down, router_weight, router_gain):
    vmem, dma = pltpu.VMEM, pltpu.SemaphoreType.DMA
    hbm = pl.BlockSpec(memory_space=pltpu.HBM)
    inside = pl.BlockSpec(memory_space=pltpu.VMEM)
    served = (16, 32, 2048)
    found = pl.pallas_call(
        exchange,
        out_shape=[vmem(served, BF16)] * 3
        + [vmem((2, JOBS, 1, 128), F32), vmem((64, 2048), BF16)],
        in_specs=[hbm] * 8,
        out_specs=[inside] * 5,
        scratch_shapes=[
            vmem((JOBS, 128, 1024), F32), vmem((JOBS, 128, 1024), BF16), vmem((JOBS, 1024, 128), BF16),
            vmem((JOBS, BLOCKS, 1, 128), F32), vmem((JOBS, BLOCKS, 1, 128), F32),
            vmem((JOBS, 64, 1024), F32), vmem((JOBS, 64, 1024), BF16),
        ]
        + [vmem((JOBS, BLOCKS, 128), F32)] * 3
        + [
            vmem((CHIPS, 2, BLOCKS, 128), F32), vmem((CHIPS, 2, BLOCKS, 128), F32),
        ]
        + [vmem((CHIPS, 2, 1, 128), F32)] * 3
        + [vmem((CHIPS, BLOCKS, 128), F32)] * 3
        + [
            vmem((2, 16, 64), F32), vmem((2, 1, 64), F32), vmem((16, 128), BF16),
            dma((6, 2)), dma((5, 2)), dma((6, 2)), dma((6, 2)), dma((4,)), dma((4,)), dma((4,)),
            dma((4,)), dma((2,)), dma((2,)), dma((2,)), dma((2,)), dma((2, 2)),
        ],
        compiler_params=pltpu.CompilerParams(
            collective_id=0, has_side_effects=True, vmem_limit_bytes=48 << 20
        ),
        name="exchange",
    )(
        w_gate, avg_gate, w_up, avg_up, jnp.swapaxes(w_down, 1, 2), jnp.swapaxes(avg_down, 1, 2),
        router_weight.T, router_gain[None, :],
    )
    out = pl.BlockSpec(memory_space=pl.ANY)
    gate, up, down, s_gate, s_up, s_down, router = pl.pallas_call(
        write_out,
        out_shape=[jax.ShapeDtypeStruct(served, BF16)] * 3
        + [jax.ShapeDtypeStruct((16, 32), F32)] * 3
        + [jax.ShapeDtypeStruct((64, 2048), BF16)],
        in_specs=[inside] * 5,
        out_specs=[out] * 7,
        scratch_shapes=[vmem((3, 16, 32), F32), dma((7,))],
        compiler_params=pltpu.CompilerParams(vmem_limit_bytes=8 << 20),
        name="write_out",
    )(*(pltpu.with_memory_space_constraint(x, pltpu.VMEM) for x in found))
    return (
        jnp.swapaxes(gate, 1, 2), jnp.swapaxes(up, 1, 2), down, s_gate, s_up, s_down, router.T,
    )


def solution(mesh):
    return jax.shard_map(
        shards,
        mesh=mesh,
        in_specs=(
            P("owner", "rows", None),
            P("owner", "rows", None),
            P("owner", "rows", None),
            P("owner", "rows", None),
            P("owner", None, "rows"),
            P("owner", None, "rows"),
            P("rows", "owner"),
            P("rows"),
        ),
        out_specs=(
            P("owner", None, "rows"),
            P("owner", None, "rows"),
            P("owner", "rows", None),
            P("owner", "rows"),
            P("owner", "rows"),
            P("owner", "rows"),
            P(),
        ),
        check_vma=False,
    )
```

```python
import jax
import jax.numpy as jnp
from jax import lax
from jax.experimental import pallas as pl
from jax.experimental.pallas import tpu as pltpu
from jax.sharding import PartitionSpec as P

MESH = pl.DeviceIdType.MESH
F32, BF16 = jnp.float32, jnp.bfloat16

SIDE = 4
CHIPS = 16
HALF = 8
JOBS = 24
BLOCKS = 8

ORDER = (10, 1, 4, 3, 12, 6, 9, 5, 15, 14, 11, 7, 13, 2, 8)
LOADS = ((0, 1), (1, 3), (4, 4), (8, 8), (16, 8))
SUMS = ((0, 1), (1, 3), (4, 4), (8, 16))


def exchange(*refs):
    (w_gate, a_gate, w_up, a_up, w_down, a_down, r_weight, r_gain) = refs[:8]
    (o_gate, o_up, o_down, o_scale, o_router) = refs[8:13]
    (wide, narrow, ready, scale, inverse, near_w, near_a, kept, given, taken) = refs[13:23]
    (all0, all1, part2, got2, sum2, part3, got3, sum3) = refs[23:31]
    (rw, rg, tile, load_sem, near_sem, trade_out, trade_in, sum_out, sum_in, ready_sem, tot_in,
     done_sem, route_sem, line_sem, scale_sem, near_share) = refs[31:]
    weights, changes, outs = (w_gate, w_up, w_down), (a_gate, a_up, a_down), (o_gate, o_up, o_down)
    owner, row = lax.axis_index("owner"), lax.axis_index("rows")
    chip, core = row // 2, row % 2
    z, y = chip // SIDE, chip % SIDE
    other = 1 - core
    partner_row = chip * 2 + other
    partner = (owner, partner_row)

    def chip_at(k):
        return (z + k // SIDE) % SIDE * SIDE + (y + k % SIDE) % SIDE

    def rows_of(which):
        return pl.ds(pl.multiple_of(which * 64, 64), 64)

    def to_partner(src, dst, out_sem, in_sem):
        return pltpu.make_async_remote_copy(
            src_ref=src, dst_ref=dst, send_sem=out_sem, recv_sem=in_sem, device_id=partner,
            device_id_type=MESH,
        )

    def sources(g):
        first, n = LOADS[g]
        m, e = first // HALF, first % HALF
        return first, n, e, ((weights[m], wide), (changes[m], narrow))

    def loads(g):
        first, n, e, pairs = sources(g)
        return [
            pltpu.make_async_copy(
                src.at[pl.ds(core * HALF + e, n)], dst.at[pl.ds(first, n), rows_of(core), :], load_sem.at[g, i]
            )
            for i, (src, dst) in enumerate(pairs)
        ]

    def near_loads(g):
        first, n, e, pairs = sources(g)
        return [
            pltpu.make_async_copy(
                src.at[pl.ds(other * HALF + e, n)], dst.at[pl.ds(first, n)], near_sem.at[g, i]
            )
            for i, ((src, _), dst) in enumerate(zip(pairs, (near_w, near_a)))
        ]

    def trades(g):
        first, n, e, pairs = sources(g)
        return [
            to_partner(
                src.at[pl.ds(other * HALF + e, n)], dst.at[pl.ds(first, n), rows_of(core), :],
                trade_out.at[g, i], trade_in.at[g, i],
            )
            for i, (src, dst) in enumerate(pairs)
        ]

    last = len(LOADS)
    route_local = [
        pltpu.make_async_copy(src, dst.at[core], load_sem.at[last, i])
        for i, (src, dst) in enumerate(((r_weight, rw), (r_gain, rg)))
    ]
    route_trade = [
        to_partner(src, dst.at[core], trade_out.at[last, i], trade_in.at[last, i])
        for i, (src, dst) in enumerate(((r_weight, rw), (r_gain, rg)))
    ]

    for copy in loads(0) + near_loads(0):
        copy.start()

    barrier = pltpu.get_barrier_semaphore()

    def greet(k, carry):
        for c in range(2):
            pl.semaphore_signal(
                barrier, inc=1, device_id=(owner, chip_at(CHIPS - k) * 2 + c), device_id_type=MESH
            )
        return carry

    lax.fori_loop(1, CHIPS, greet, 0)
    for k in range(1, SIDE):
        for c in range(2):
            pl.semaphore_signal(
                barrier, inc=1, device_id=((owner + k) % SIDE, chip * 2 + c), device_id_type=MESH
            )
    pl.semaphore_signal(barrier, inc=1, device_id=partner, device_id_type=MESH)

    for g in range(1, len(LOADS)):
        for copy in loads(g) + near_loads(g):
            copy.start()
    for copy in route_local:
        copy.start()

    def lanes_of(b):
        return slice(b * 128, (b + 1) * 128)

    def squares(x):
        return jnp.sum(x * x, axis=0, keepdims=True)

    def own_rows(g):
        first, n = LOADS[g]
        for copy in loads(g) + near_loads(g):
            copy.wait()

        def one(job, carry):
            for b in range(BLOCKS):
                lanes = lanes_of(b)
                given[job, b : b + 1, :] = squares(near_w[job, :, lanes] + near_a[job, :, lanes].astype(F32))
                kept[job, b : b + 1, :] = squares(
                    wide[job, rows_of(core), lanes] + narrow[job, rows_of(core), lanes].astype(F32)
                )
            return carry

        lax.fori_loop(first, first + n, one, 0)

    def shared(k, first, n):
        jobs = pl.ds(first, n)
        return to_partner(given.at[jobs], taken.at[jobs], near_share.at[k, 0], near_share.at[k, 1])

    near = [shared(0, 1, 3), shared(1, 4, 4), shared(2, 8, 16)]
    own_rows(0)

    pl.semaphore_wait(barrier, 1 + 2 * (CHIPS - 1) + 2 * (SIDE - 1))

    def traded(g):
        for copy in trades(g):
            copy.wait_recv()

    def to_chips(src, dst, out_sem, in_sem):
        def go(k, carry):
            there = chip_at(k)
            pltpu.make_async_remote_copy(
                src_ref=src(there), dst_ref=dst, send_sem=out_sem, recv_sem=in_sem,
                device_id=(owner, there * 2 + core), device_id_type=MESH,
            ).start()
            return carry

        lax.fori_loop(1, CHIPS, go, 0)

    def wait_for(ref, sem):
        pltpu.make_async_copy(ref, ref, sem).wait()

    def keep(job, b, total):
        root = jnp.sqrt(total)
        scale[job, b] = root
        inverse[job, b] = 1.0 / root

    def sums_from_all(g, got):
        def send(src, to):
            pltpu.make_async_remote_copy(
                src_ref=src.at[0], dst_ref=got.at[row], send_sem=sum_out.at[g], recv_sem=sum_in.at[g],
                device_id=(owner, to), device_id_type=MESH,
            ).start()

        def go(k, carry):
            there = chip_at(CHIPS - k)
            send(kept, there * 2 + core)
            send(given, there * 2 + other)
            return carry

        lax.fori_loop(1, CHIPS, go, 0)
        send(given, partner_row)
        got[row] = kept[0]

    def sums_from_all_added(g, got):
        wait_for(got.at[pl.ds(0, 2 * CHIPS - 1)], sum_in.at[g])
        total = got[0]
        for s in range(1, 2 * CHIPS):
            total = total + got[s]
        for b in range(BLOCKS):
            keep(0, b, total[b : b + 1, :])

    def sums_broadcast(g, got):
        first, n = SUMS[g]
        for i in range(n):
            got[chip, i] = kept[first + i] + taken[first + i]
        to_chips(lambda there: got.at[chip], got.at[chip], sum_out.at[g], sum_in.at[g])

    def sums_added(g, got):
        first, n = SUMS[g]
        wait_for(got.at[pl.ds(0, CHIPS - 1)], sum_in.at[g])
        for i in range(n):
            total = got[0, i]
            for s in range(1, CHIPS):
                total = total + got[s, i]
            for b in range(BLOCKS):
                keep(first + i, b, total[b : b + 1, :])

    def sums_scattered(g, part, got):
        first, n = SUMS[g]
        per = n // 2

        def one(i, carry):
            total = kept[first + i] + taken[first + i]
            if n == CHIPS:
                part[i] = total
                return carry
            for b in range(BLOCKS):
                line = i * BLOCKS + b
                part[line // per, line % per] = total[b : b + 1, :]
            return carry

        lax.fori_loop(0, n, one, 0)
        got[chip] = part[chip]
        to_chips(lambda there: part.at[there], got.at[chip], sum_out.at[g], sum_in.at[g])

    def sums_gathered(g, got, whole):
        wait_for(got.at[pl.ds(0, CHIPS - 1)], sum_in.at[g])
        total = got[0]
        for s in range(1, CHIPS):
            total = total + got[s]
        whole[chip] = total
        to_chips(lambda there: whole.at[chip], whole.at[chip], ready_sem.at[g], tot_in.at[g])

    def sums_taken(g, whole):
        first, n = SUMS[g]
        per = n // 2
        wait_for(whole.at[pl.ds(0, CHIPS - 1)], tot_in.at[g])

        def one(i, carry):
            for b in range(BLOCKS):
                line = i * BLOCKS + b
                keep(first + i, b, whole[i, b : b + 1, :] if n == CHIPS else whole[line // per, line % per])
            return carry

        lax.fori_loop(0, n, one, 0)

    mine = pl.ds(pl.multiple_of(chip * 128, 128), 128)

    def lines_for(which):
        return pl.ds(pl.multiple_of(which * 32, 32), 32)

    def to_all(send):
        for k in ORDER:
            there = chip_at(k)
            for t in range(2):
                send(there * 2 + (core + t) % 2)
        send(partner_row)

    def normalise(job):
        def blocks(b, carry):
            lanes = pl.ds(pl.multiple_of(b * 128, 128), 128)
            x = wide[job, :, lanes] + narrow[job, :, lanes].astype(F32)
            ready[job, lanes, :] = (x * inverse[job, b]).astype(BF16).T
            return carry

        lax.fori_loop(0, BLOCKS, blocks, 0)

    def issue(m, job):
        at = core * HALF + job - m * HALF

        def send(to):
            pltpu.make_async_remote_copy(
                src_ref=ready.at[job, lines_for(to), :], dst_ref=outs[m].at[at, :, mine],
                send_sem=done_sem.at[0], recv_sem=done_sem.at[1], device_id=(owner, to), device_id_type=MESH,
            ).start()

        to_all(send)
        outs[m][at, :, mine] = ready[job, lines_for(row), :]

    def sends(m, first, n):
        def one(i, carry):
            normalise(first + i)
            issue(m, first + i)
            return carry

        lax.fori_loop(0, n, one, 0)

    lines = pl.ds(pl.multiple_of(owner * 16 + core * HALF, HALF), HALF)

    def router_tile():
        for copy in route_local:
            copy.wait()
        for copy in route_trade:
            copy.wait_recv()
        folded = jnp.concatenate([rw[c] * rg[c] for c in range(2)], axis=1).astype(BF16)
        tile[...] = folded
        for_core = pl.ds(pl.multiple_of(core * HALF, HALF), HALF)
        o_router[lines, mine] = jnp.where(core == 0, folded[:HALF], folded[HALF:])
        to_chips(lambda there: tile.at[for_core], o_router.at[lines, mine], route_sem.at[0], route_sem.at[1])

    def router_lines():
        wait_for(o_router.at[pl.ds(0, HALF), pl.ds(0, 15 * 128)], route_sem.at[1])
        for k in range(SIDE):
            for c in range(2):
                if k == 0 and c == 0:
                    continue
                to = ((owner + k) % SIDE, chip * 2 + (core + c) % 2)
                pltpu.make_async_remote_copy(
                    src_ref=o_router.at[lines, :], dst_ref=o_router.at[lines, :], send_sem=line_sem.at[0],
                    recv_sem=line_sem.at[1], device_id=to, device_id_type=MESH,
                ).start()

    sums_from_all(0, all0)
    own_rows(1)
    near[0].start()
    for copy in trades(0) + route_trade:
        copy.start()
    own_rows(2)
    near[1].start()
    for copy in trades(1):
        copy.start()
    near[0].wait_recv()
    sums_broadcast(1, all1)
    near[1].wait_recv()
    sums_scattered(2, part2, got2)
    own_rows(3)
    own_rows(4)
    near[2].start()
    for copy in trades(2) + trades(3) + trades(4):
        copy.start()
    traded(0)
    sums_from_all_added(0, all0)
    sends(0, 0, 1)
    near[2].wait_recv()
    sums_scattered(3, part3, got3)
    traded(1)
    sums_added(1, all1)
    normalise(1)
    sums_gathered(2, got2, sum2)
    issue(0, 1)
    sends(0, 2, 2)
    router_tile()
    traded(2)
    sums_taken(2, sum2)
    normalise(4)
    sums_gathered(3, got3, sum3)
    issue(0, 4)
    sends(0, 5, 3)
    traded(3)
    sums_taken(3, sum3)
    sends(1, 8, 8)
    router_lines()
    traded(4)
    sends(2, 16, 8)

    o_scale[core] = scale[:, chip // 2]
    share = to_partner(scale.at[:, chip // 2], o_scale.at[core], scale_sem.at[0], scale_sem.at[1])
    share.start()

    for copy in near:
        copy.wait_send()
    for g in range(len(LOADS)):
        for copy in trades(g):
            copy.wait_send()
    for copy in route_trade:
        copy.wait_send()
    for g, got in enumerate((all0, all1, got2, got3)):
        wait_for(got.at[pl.ds(0, got.shape[0] - 1)], sum_out.at[g])
    for g, whole in ((2, sum2), (3, sum3)):
        wait_for(whole.at[pl.ds(0, CHIPS - 1)], ready_sem.at[g])
    wait_for(o_router.at[pl.ds(0, HALF), pl.ds(0, 15 * 128)], route_sem.at[0])
    for s in range(2):
        wait_for(o_router.at[pl.ds(0, 56), :], line_sem.at[s])
    share.wait()
    for s in range(2):
        wait_for(ready.at[:, pl.ds(0, 31 * 32), :], done_sem.at[s])


def write_out(*refs):
    (gate, up, down, scale, router, o_gate, o_up, o_down, *rest) = refs
    (*o_scales, o_router, lines, sem) = rest
    large = [
        pltpu.make_async_copy(src, dst, sem.at[i])
        for i, (src, dst) in enumerate(((gate, o_gate), (up, o_up), (down, o_down), (router, o_router)))
    ]
    for copy in large:
        copy.start()
    row = lax.axis_index("rows")
    for m in range(3):
        for c in range(2):
            block = scale[c, m * HALF : (m + 1) * HALF, 0, :]
            block = pltpu.roll(block, (128 - row % 4 * 32) % 128, 1)
            lines[m, c * HALF : (c + 1) * HALF, :] = block[:, :32]
    small = [pltpu.make_async_copy(lines.at[m], out, sem.at[4 + m]) for m, out in enumerate(o_scales)]
    for copy in small:
        copy.start()
    for copy in large + small:
        copy.wait()


def shards(w_gate, avg_gate, w_up, avg_up, w_down, avg_down, router_weight, router_gain):
    vmem, dma = pltpu.VMEM, pltpu.SemaphoreType.DMA
    hbm = pl.BlockSpec(memory_space=pltpu.HBM)
    inside = pl.BlockSpec(memory_space=pltpu.VMEM)
    served = (16, 32, 2048)
    found = pl.pallas_call(
        exchange,
        out_shape=[vmem(served, BF16)] * 3
        + [vmem((2, JOBS, 1, 128), F32), vmem((64, 2048), BF16)],
        in_specs=[hbm] * 8,
        out_specs=[inside] * 5,
        scratch_shapes=[
            vmem((JOBS, 128, 1024), F32), vmem((JOBS, 128, 1024), BF16), vmem((JOBS, 1024, 128), BF16),
            vmem((JOBS, BLOCKS, 1, 128), F32), vmem((JOBS, BLOCKS, 1, 128), F32),
            vmem((JOBS, 64, 1024), F32), vmem((JOBS, 64, 1024), BF16),
        ]
        + [vmem((JOBS, BLOCKS, 128), F32)] * 3
        + [
            vmem((2 * CHIPS, BLOCKS, 128), F32), vmem((CHIPS, 3, BLOCKS, 128), F32),
        ]
        + [vmem((CHIPS, 2, 1, 128), F32)] * 3
        + [vmem((CHIPS, BLOCKS, 128), F32)] * 3
        + [
            vmem((2, 16, 64), F32), vmem((2, 1, 64), F32), vmem((16, 128), BF16),
            dma((6, 2)), dma((5, 2)), dma((6, 2)), dma((6, 2)), dma((4,)), dma((4,)), dma((4,)),
            dma((4,)), dma((2,)), dma((2,)), dma((2,)), dma((2,)), dma((3, 2)),
        ],
        compiler_params=pltpu.CompilerParams(
            collective_id=0, has_side_effects=True, vmem_limit_bytes=48 << 20
        ),
        name="exchange",
    )(
        w_gate, avg_gate, w_up, avg_up, jnp.swapaxes(w_down, 1, 2), jnp.swapaxes(avg_down, 1, 2),
        router_weight.T, router_gain[None, :],
    )
    out = pl.BlockSpec(memory_space=pl.ANY)
    gate, up, down, s_gate, s_up, s_down, router = pl.pallas_call(
        write_out,
        out_shape=[jax.ShapeDtypeStruct(served, BF16)] * 3
        + [jax.ShapeDtypeStruct((16, 32), F32)] * 3
        + [jax.ShapeDtypeStruct((64, 2048), BF16)],
        in_specs=[inside] * 5,
        out_specs=[out] * 7,
        scratch_shapes=[vmem((3, 16, 32), F32), dma((7,))],
        compiler_params=pltpu.CompilerParams(vmem_limit_bytes=8 << 20),
        name="write_out",
    )(*(pltpu.with_memory_space_constraint(x, pltpu.VMEM) for x in found))
    return (
        jnp.swapaxes(gate, 1, 2), jnp.swapaxes(up, 1, 2), down, s_gate, s_up, s_down, router.T,
    )


def solution(mesh):
    return jax.shard_map(
        shards,
        mesh=mesh,
        in_specs=(
            P("owner", "rows", None),
            P("owner", "rows", None),
            P("owner", "rows", None),
            P("owner", "rows", None),
            P("owner", None, "rows"),
            P("owner", None, "rows"),
            P("rows", "owner"),
            P("rows"),
        ),
        out_specs=(
            P("owner", None, "rows"),
            P("owner", None, "rows"),
            P("owner", "rows", None),
            P("owner", "rows"),
            P("owner", "rows"),
            P("owner", "rows"),
            P(),
        ),
        check_vma=False,
    )
```

```python
import jax
import jax.numpy as jnp
from jax import lax
from jax.experimental import pallas as pl
from jax.experimental.pallas import tpu as pltpu
from jax.sharding import PartitionSpec as P

MESH = pl.DeviceIdType.MESH
F32, BF16 = jnp.float32, jnp.bfloat16

SIDE = 4
CHIPS = 16
HALF = 8
JOBS = 24
BLOCKS = 8

ORDER = (10, 1, 4, 3, 12, 6, 9, 5, 15, 14, 11, 7, 13, 2, 8)
FAR = (10, 14, 11, 6, 9, 8, 2, 13, 7, 15, 5, 12, 3, 4, 1)

LOADS = ((0, 1), (1, 3), (4, 4), (8, 8), (16, 8))
SUMS = ((0, 1), (1, 3), (4, 4), (8, 16))


def exchange(*refs):
    (w_gate, a_gate, w_up, a_up, w_down, a_down, r_weight, r_gain) = refs[:8]
    (o_gate, o_up, o_down, o_scale, o_router) = refs[8:13]
    (wide, narrow, ready, scale, inverse, near_w, near_a, kept, given, taken) = refs[13:23]
    (all0, all1, part2, got2, sum2, part3, got3, sum3) = refs[23:31]
    (rw, rg, tile, load_sem, near_sem, trade_out, trade_in, sum_out, sum_in, ready_sem, tot_in,
     done_sem, route_sem, line_sem, scale_sem, near_share) = refs[31:]
    weights, changes, outs = (w_gate, w_up, w_down), (a_gate, a_up, a_down), (o_gate, o_up, o_down)
    owner, row = lax.axis_index("owner"), lax.axis_index("rows")
    chip, core = row // 2, row % 2
    z, y = chip // SIDE, chip % SIDE
    other = 1 - core
    partner_row = chip * 2 + other
    partner = (owner, partner_row)

    def chip_at(k):
        return (z + k // SIDE) % SIDE * SIDE + (y + k % SIDE) % SIDE

    def rows_of(which):
        return pl.ds(pl.multiple_of(which * 64, 64), 64)

    def to_partner(src, dst, out_sem, in_sem):
        return pltpu.make_async_remote_copy(
            src_ref=src, dst_ref=dst, send_sem=out_sem, recv_sem=in_sem, device_id=partner,
            device_id_type=MESH,
        )

    def sources(g):
        first, n = LOADS[g]
        m, e = first // HALF, first % HALF
        return first, n, e, ((weights[m], wide), (changes[m], narrow))

    def loads(g):
        first, n, e, pairs = sources(g)
        return [
            pltpu.make_async_copy(
                src.at[pl.ds(core * HALF + e, n)], dst.at[pl.ds(first, n), rows_of(core), :], load_sem.at[g, i]
            )
            for i, (src, dst) in enumerate(pairs)
        ]

    def near_loads(g):
        first, n, e, pairs = sources(g)
        return [
            pltpu.make_async_copy(
                src.at[pl.ds(other * HALF + e, n)], dst.at[pl.ds(first, n)], near_sem.at[g, i]
            )
            for i, ((src, _), dst) in enumerate(zip(pairs, (near_w, near_a)))
        ]

    def trades(g):
        first, n, e, pairs = sources(g)
        return [
            to_partner(
                src.at[pl.ds(other * HALF + e, n)], dst.at[pl.ds(first, n), rows_of(core), :],
                trade_out.at[g, i], trade_in.at[g, i],
            )
            for i, (src, dst) in enumerate(pairs)
        ]

    last = len(LOADS)
    route_local = [
        pltpu.make_async_copy(src, dst.at[core], load_sem.at[last, i])
        for i, (src, dst) in enumerate(((r_weight, rw), (r_gain, rg)))
    ]
    route_trade = [
        to_partner(src, dst.at[core], trade_out.at[last, i], trade_in.at[last, i])
        for i, (src, dst) in enumerate(((r_weight, rw), (r_gain, rg)))
    ]

    for copy in loads(0) + near_loads(0):
        copy.start()

    barrier = pltpu.get_barrier_semaphore()

    for k in FAR:
        for c in range(2):
            pl.semaphore_signal(
                barrier, inc=1, device_id=(owner, chip_at(k) * 2 + c), device_id_type=MESH
            )
    for k in range(1, SIDE):
        for c in range(2):
            pl.semaphore_signal(
                barrier, inc=1, device_id=((owner + k) % SIDE, chip * 2 + c), device_id_type=MESH
            )
    pl.semaphore_signal(barrier, inc=1, device_id=partner, device_id_type=MESH)

    for g in range(1, len(LOADS)):
        for copy in loads(g) + near_loads(g):
            copy.start()
    for copy in route_local:
        copy.start()

    def lanes_of(b):
        return slice(b * 128, (b + 1) * 128)

    def squares(x):
        return jnp.sum(x * x, axis=0, keepdims=True)

    def own_rows(g):
        first, n = LOADS[g]
        for copy in loads(g) + near_loads(g):
            copy.wait()

        def one(job, carry):
            for b in range(BLOCKS):
                lanes = lanes_of(b)
                given[job, b : b + 1, :] = squares(near_w[job, :, lanes] + near_a[job, :, lanes].astype(F32))
                kept[job, b : b + 1, :] = squares(
                    wide[job, rows_of(core), lanes] + narrow[job, rows_of(core), lanes].astype(F32)
                )
            return carry

        lax.fori_loop(first, first + n, one, 0)

    def shared(k, first, n):
        jobs = pl.ds(first, n)
        return to_partner(given.at[jobs], taken.at[jobs], near_share.at[k, 0], near_share.at[k, 1])

    near = [shared(0, 1, 3), shared(1, 4, 4), shared(2, 8, 16)]
    own_rows(0)

    pl.semaphore_wait(barrier, 1 + 2 * (CHIPS - 1) + 2 * (SIDE - 1))

    def traded(g):
        for copy in trades(g):
            copy.wait_recv()

    def to_chips(src, dst, out_sem, in_sem):
        for k in FAR:
            there = chip_at(k)
            pltpu.make_async_remote_copy(
                src_ref=src(there), dst_ref=dst, send_sem=out_sem, recv_sem=in_sem,
                device_id=(owner, there * 2 + core), device_id_type=MESH,
            ).start()

    def wait_for(ref, sem):
        pltpu.make_async_copy(ref, ref, sem).wait()

    def keep(job, b, total):
        root = jnp.sqrt(total)
        scale[job, b] = root
        inverse[job, b] = 1.0 / root

    def sums_from_all(g, got):
        def send(src, to):
            pltpu.make_async_remote_copy(
                src_ref=src.at[0], dst_ref=got.at[row], send_sem=sum_out.at[g], recv_sem=sum_in.at[g],
                device_id=(owner, to), device_id_type=MESH,
            ).start()

        for k in FAR:
            there = chip_at(k)
            send(kept, there * 2 + core)
            send(given, there * 2 + other)
        send(given, partner_row)
        got[row] = kept[0]

    def sums_from_all_added(g, got):
        wait_for(got.at[pl.ds(0, 2 * CHIPS - 1)], sum_in.at[g])
        total = got[0]
        for s in range(1, 2 * CHIPS):
            total = total + got[s]
        for b in range(BLOCKS):
            keep(0, b, total[b : b + 1, :])

    def sums_broadcast(g, got):
        first, n = SUMS[g]
        for i in range(n):
            got[chip, i] = kept[first + i] + taken[first + i]
        to_chips(lambda there: got.at[chip], got.at[chip], sum_out.at[g], sum_in.at[g])

    def sums_added(g, got):
        first, n = SUMS[g]
        wait_for(got.at[pl.ds(0, CHIPS - 1)], sum_in.at[g])
        for i in range(n):
            total = got[0, i]
            for s in range(1, CHIPS):
                total = total + got[s, i]
            for b in range(BLOCKS):
                keep(first + i, b, total[b : b + 1, :])

    def sums_scattered(g, part, got):
        first, n = SUMS[g]
        per = n // 2

        def one(i, carry):
            total = kept[first + i] + taken[first + i]
            if n == CHIPS:
                part[i] = total
                return carry
            for b in range(BLOCKS):
                line = i * BLOCKS + b
                part[line // per, line % per] = total[b : b + 1, :]
            return carry

        lax.fori_loop(0, n, one, 0)
        got[chip] = part[chip]
        to_chips(lambda there: part.at[there], got.at[chip], sum_out.at[g], sum_in.at[g])

    def sums_gathered(g, got, whole):
        wait_for(got.at[pl.ds(0, CHIPS - 1)], sum_in.at[g])
        total = got[0]
        for s in range(1, CHIPS):
            total = total + got[s]
        whole[chip] = total
        to_chips(lambda there: whole.at[chip], whole.at[chip], ready_sem.at[g], tot_in.at[g])

    def sums_taken(g, whole):
        first, n = SUMS[g]
        per = n // 2
        wait_for(whole.at[pl.ds(0, CHIPS - 1)], tot_in.at[g])

        def one(i, carry):
            for b in range(BLOCKS):
                line = i * BLOCKS + b
                keep(first + i, b, whole[i, b : b + 1, :] if n == CHIPS else whole[line // per, line % per])
            return carry

        lax.fori_loop(0, n, one, 0)

    mine = pl.ds(pl.multiple_of(chip * 128, 128), 128)

    def lines_for(which):
        return pl.ds(pl.multiple_of(which * 32, 32), 32)

    def to_all(send):
        for k in ORDER:
            there = chip_at(k)
            for t in range(2):
                send(there * 2 + (core + t) % 2)
        send(partner_row)

    def normalise(job):
        def blocks(b, carry):
            lanes = pl.ds(pl.multiple_of(b * 128, 128), 128)
            x = wide[job, :, lanes] + narrow[job, :, lanes].astype(F32)
            ready[job, lanes, :] = (x * inverse[job, b]).astype(BF16).T
            return carry

        lax.fori_loop(0, BLOCKS, blocks, 0)

    def issue(m, job):
        at = core * HALF + job - m * HALF

        def send(to):
            pltpu.make_async_remote_copy(
                src_ref=ready.at[job, lines_for(to), :], dst_ref=outs[m].at[at, :, mine],
                send_sem=done_sem.at[0], recv_sem=done_sem.at[1], device_id=(owner, to), device_id_type=MESH,
            ).start()

        to_all(send)
        outs[m][at, :, mine] = ready[job, lines_for(row), :]

    def sends(m, first, n):
        def one(i, carry):
            normalise(first + i)
            issue(m, first + i)
            return carry

        lax.fori_loop(0, n, one, 0)

    lines = pl.ds(pl.multiple_of(owner * 16 + core * HALF, HALF), HALF)

    def router_tile():
        for copy in route_local:
            copy.wait()
        for copy in route_trade:
            copy.wait_recv()
        folded = jnp.concatenate([rw[c] * rg[c] for c in range(2)], axis=1).astype(BF16)
        tile[...] = folded
        for_core = pl.ds(pl.multiple_of(core * HALF, HALF), HALF)
        o_router[lines, mine] = jnp.where(core == 0, folded[:HALF], folded[HALF:])
        to_chips(lambda there: tile.at[for_core], o_router.at[lines, mine], route_sem.at[0], route_sem.at[1])

    def router_lines():
        wait_for(o_router.at[pl.ds(0, HALF), pl.ds(0, 15 * 128)], route_sem.at[1])
        for k in range(SIDE):
            for c in range(2):
                if k == 0 and c == 0:
                    continue
                to = ((owner + k) % SIDE, chip * 2 + (core + c) % 2)
                pltpu.make_async_remote_copy(
                    src_ref=o_router.at[lines, :], dst_ref=o_router.at[lines, :], send_sem=line_sem.at[0],
                    recv_sem=line_sem.at[1], device_id=to, device_id_type=MESH,
                ).start()

    sums_from_all(0, all0)
    own_rows(1)
    near[0].start()
    for copy in trades(0) + route_trade:
        copy.start()
    own_rows(2)
    near[1].start()
    for copy in trades(1):
        copy.start()
    near[0].wait_recv()
    sums_broadcast(1, all1)
    near[1].wait_recv()
    sums_scattered(2, part2, got2)
    own_rows(3)
    own_rows(4)
    near[2].start()
    for copy in trades(2) + trades(3) + trades(4):
        copy.start()
    traded(0)
    sums_from_all_added(0, all0)
    sends(0, 0, 1)
    near[2].wait_recv()
    sums_scattered(3, part3, got3)
    traded(1)
    sums_added(1, all1)
    normalise(1)
    sums_gathered(2, got2, sum2)
    issue(0, 1)
    sends(0, 2, 2)
    router_tile()
    traded(2)
    sums_taken(2, sum2)
    normalise(4)
    sums_gathered(3, got3, sum3)
    issue(0, 4)
    sends(0, 5, 3)
    traded(3)
    sums_taken(3, sum3)
    sends(1, 8, 8)
    router_lines()
    traded(4)
    sends(2, 16, 8)

    o_scale[core] = scale[:, chip // 2]
    share = to_partner(scale.at[:, chip // 2], o_scale.at[core], scale_sem.at[0], scale_sem.at[1])
    share.start()

    for copy in near:
        copy.wait_send()
    for g in range(len(LOADS)):
        for copy in trades(g):
            copy.wait_send()
    for copy in route_trade:
        copy.wait_send()
    for g, got in enumerate((all0, all1, got2, got3)):
        wait_for(got.at[pl.ds(0, got.shape[0] - 1)], sum_out.at[g])
    for g, whole in ((2, sum2), (3, sum3)):
        wait_for(whole.at[pl.ds(0, CHIPS - 1)], ready_sem.at[g])
    wait_for(o_router.at[pl.ds(0, HALF), pl.ds(0, 15 * 128)], route_sem.at[0])
    for s in range(2):
        wait_for(o_router.at[pl.ds(0, 56), :], line_sem.at[s])
    share.wait()
    for s in range(2):
        wait_for(ready.at[:, pl.ds(0, 31 * 32), :], done_sem.at[s])


def write_out(*refs):
    (gate, up, down, scale, router, o_gate, o_up, o_down, *rest) = refs
    (*o_scales, o_router, lines, sem) = rest
    large = [
        pltpu.make_async_copy(src, dst, sem.at[i])
        for i, (src, dst) in enumerate(((gate, o_gate), (up, o_up), (down, o_down), (router, o_router)))
    ]
    for copy in large:
        copy.start()
    row = lax.axis_index("rows")
    for m in range(3):
        for c in range(2):
            block = scale[c, m * HALF : (m + 1) * HALF, 0, :]
            block = pltpu.roll(block, (128 - row % 4 * 32) % 128, 1)
            lines[m, c * HALF : (c + 1) * HALF, :] = block[:, :32]
    small = [pltpu.make_async_copy(lines.at[m], out, sem.at[4 + m]) for m, out in enumerate(o_scales)]
    for copy in small:
        copy.start()
    for copy in large + small:
        copy.wait()


def shards(w_gate, avg_gate, w_up, avg_up, w_down, avg_down, router_weight, router_gain):
    vmem, dma = pltpu.VMEM, pltpu.SemaphoreType.DMA
    hbm = pl.BlockSpec(memory_space=pltpu.HBM)
    inside = pl.BlockSpec(memory_space=pltpu.VMEM)
    served = (16, 32, 2048)
    found = pl.pallas_call(
        exchange,
        out_shape=[vmem(served, BF16)] * 3
        + [vmem((2, JOBS, 1, 128), F32), vmem((64, 2048), BF16)],
        in_specs=[hbm] * 8,
        out_specs=[inside] * 5,
        scratch_shapes=[
            vmem((JOBS, 128, 1024), F32), vmem((JOBS, 128, 1024), BF16), vmem((JOBS, 1024, 128), BF16),
            vmem((JOBS, BLOCKS, 1, 128), F32), vmem((JOBS, BLOCKS, 1, 128), F32),
            vmem((JOBS, 64, 1024), F32), vmem((JOBS, 64, 1024), BF16),
        ]
        + [vmem((JOBS, BLOCKS, 128), F32)] * 3
        + [
            vmem((2 * CHIPS, BLOCKS, 128), F32), vmem((CHIPS, 3, BLOCKS, 128), F32),
        ]
        + [vmem((CHIPS, 2, 1, 128), F32)] * 3
        + [vmem((CHIPS, BLOCKS, 128), F32)] * 3
        + [
            vmem((2, 16, 64), F32), vmem((2, 1, 64), F32), vmem((16, 128), BF16),
            dma((6, 2)), dma((5, 2)), dma((6, 2)), dma((6, 2)), dma((4,)), dma((4,)), dma((4,)),
            dma((4,)), dma((2,)), dma((2,)), dma((2,)), dma((2,)), dma((3, 2)),
        ],
        compiler_params=pltpu.CompilerParams(
            collective_id=0, has_side_effects=True, vmem_limit_bytes=48 << 20
        ),
        name="exchange",
    )(
        w_gate, avg_gate, w_up, avg_up, jnp.swapaxes(w_down, 1, 2), jnp.swapaxes(avg_down, 1, 2),
        router_weight.T, router_gain[None, :],
    )
    out = pl.BlockSpec(memory_space=pl.ANY)
    gate, up, down, s_gate, s_up, s_down, router = pl.pallas_call(
        write_out,
        out_shape=[jax.ShapeDtypeStruct(served, BF16)] * 3
        + [jax.ShapeDtypeStruct((16, 32), F32)] * 3
        + [jax.ShapeDtypeStruct((64, 2048), BF16)],
        in_specs=[inside] * 5,
        out_specs=[out] * 7,
        scratch_shapes=[vmem((3, 16, 32), F32), dma((7,))],
        compiler_params=pltpu.CompilerParams(vmem_limit_bytes=8 << 20),
        name="write_out",
    )(*(pltpu.with_memory_space_constraint(x, pltpu.VMEM) for x in found))
    return (
        jnp.swapaxes(gate, 1, 2), jnp.swapaxes(up, 1, 2), down, s_gate, s_up, s_down, router.T,
    )


def solution(mesh):
    return jax.shard_map(
        shards,
        mesh=mesh,
        in_specs=(
            P("owner", "rows", None),
            P("owner", "rows", None),
            P("owner", "rows", None),
            P("owner", "rows", None),
            P("owner", None, "rows"),
            P("owner", None, "rows"),
            P("rows", "owner"),
            P("rows"),
        ),
        out_specs=(
            P("owner", None, "rows"),
            P("owner", None, "rows"),
            P("owner", "rows", None),
            P("owner", "rows"),
            P("owner", "rows"),
            P("owner", "rows"),
            P(),
        ),
        check_vma=False,
    )
```
